32 devices in a mesh: gx: 4 (over y, core), gy: 4 (over z), gz: 2 (over x).
Axes of the slice: x: 2, y: 2, z: 4, core: 2. Of those that a mesh axis runs over, the one named last changes fastest.
Arguments:
- positions: float32 [3, 8, 8, 4, 256], P(None, 'gx', 'gy', 'gz'), may hold values from 0 to 1
- velocities: float32 [3, 8, 8, 4, 256], P(None, 'gx', 'gy', 'gz'), may hold values from -3 to 3
- masses: float32 [8, 8, 4, 256], P('gx', 'gy', 'gz'), may hold values from 0.0025 to 0.01
- entropy: float32 [8, 8, 4, 256], P('gx', 'gy', 'gz'), may hold values from 0.5 to 2
- counts: int32 [8, 8, 4], P('gx', 'gy', 'gz'), may hold values from 8 to 256, as said below
Outputs:
- density: float32 [8, 8, 4, 256], P('gx', 'gy', 'gz')
- acceleration: float32 [3, 8, 8, 4, 256], P(None, 'gx', 'gy', 'gz')
The draws below stay inside these ranges and needn't reach their ends.
Inputs may be any that keep to these rules, and one draw needn't show every extreme that they name: The first counts[c] slots of cell c hold particles; the other slots of the cell are padding whose values are arbitrary.
All inputs are finite; a program needn't handle non-finite values.
Results may differ from the reference program's by a relative error of at most 0.0003.
Values sent between devices are 32-bit elements; how exact they have to be, the bound alone decides.
No kernel may reach another device: no remote copies, remote signals or barrier semaphores. Data moves between devices by JAX's collectives and lax.ppermute only.
A program may use at most 64 MiB of HBM per device.

```python
import math
import jax
import jax.numpy as jnp
from jax import lax

LX = 2
LY = 2
LZ = 2
PC = 256
NX = 8
NY = 8
NZ = 4
N_GX = 4
N_GY = 4
N_GZ = 2


def draw_counts(key, part):
    key_base, key_crowd, key_rare, key_half = jax.random.split(key, 4)
    base_count = jax.random.randint(key_base, (NX, NY, NZ), 8, PC // 2 + 1)
    crowded = jax.random.randint(key_crowd, (NX // LX, NY // LY, NZ // LZ), 0, 6) == 0
    crowded = jnp.repeat(jnp.repeat(jnp.repeat(crowded, LX, 0), LY, 1), LZ, 2)
    rare_full = jax.random.randint(key_rare, (NX, NY, NZ), 0, 64) == 0
    half_full = jax.random.randint(key_half, (NX, NY, NZ), 0, 2) == 0
    heavy = rare_full | crowded & half_full
    heavy = heavy.at[0, 0, 0].set(True)
    return jnp.where(heavy, PC, base_count).astype(jnp.int32)


def steps_of(rng, shape, cuts, least, top_value):
    gain, own = 1.0, jax.random.fold_in(rng, 6)
    for dim, parts in cuts:
        steps = jnp.exp(jax.random.uniform(jax.random.fold_in(own, dim), (parts,), jnp.float32, least / len(cuts), top_value / len(cuts)))
        gain = gain * jnp.repeat(steps, shape[dim] // parts).reshape([-1 if axis == dim else 1 for axis in range(len(shape))])
    return gain


def normal_values(own_key, extent, width, most, shards=(), kind=jnp.bfloat16):
    array = width * jax.random.normal(own_key, extent, jnp.float32)
    if shards:
        array = array * steps_of(own_key, extent, shards, -0.22, 0.18)
    return jnp.clip(array, -most, most).astype(kind)


def setup_inputs(seed: int = 0) -> dict:
    seeds = jax.random.split(jax.random.key(seed), 6)
    positions = jnp.clip(1.0 * jax.random.uniform(seeds[0], (3, NX, NY, NZ, PC), jnp.float32) ** steps_of(seeds[0], (3, NX, NY, NZ, PC), ((1, 4), (2, 4), (3, 2)), -0.2, 0.2), 0.0, 1.0)
    velocities = normal_values(seeds[1], (3, NX, NY, NZ, PC), 0.5, 3.0, ((1, 4), (2, 4), (3, 2)), jnp.float32)
    masses = jnp.clip(jnp.exp(math.log(0.01) - 1.3862944 * jax.random.uniform(seeds[2], (NX, NY, NZ, PC), jnp.float32) ** steps_of(seeds[2], (NX, NY, NZ, PC), ((0, 4), (1, 4), (2, 2)), -0.2, 0.2)), 0.0025, 0.01)
    entropy = jnp.clip(jnp.exp(math.log(2.0) - 1.3862944 * jax.random.uniform(seeds[3], (NX, NY, NZ, PC), jnp.float32) ** steps_of(seeds[3], (NX, NY, NZ, PC), ((0, 4), (1, 4), (2, 2)), -0.2, 0.2)), 0.5, 2.0)
    counts = draw_counts(jax.random.fold_in(seeds[5], 71), 0)
    return dict(positions=positions, velocities=velocities, masses=masses, entropy=entropy, counts=counts)


SIGMA = 8.0 / math.pi
GAMMA = 5.0 / 3.0
ALPHA = 1.0
BETA = 2.0
SOFTEN = 0.01

def kernel_value(radius_sq):
    radius = jnp.sqrt(radius_sq)
    near_part = 1.0 - 6.0 * radius * radius + 6.0 * radius * radius * radius
    far_part = 2.0 * (1.0 - radius) ** 3
    return SIGMA * jnp.where(radius < 0.5, near_part, jnp.where(radius < 1.0, far_part, 0.0))

def kernel_slope(radius_sq):
    radius = jnp.sqrt(radius_sq)
    near_part = -12.0 + 18.0 * radius
    far_part = -6.0 * (1.0 - radius) ** 2 / jnp.maximum(radius, 0.5)
    return SIGMA * jnp.where(radius < 0.5, near_part, jnp.where(radius < 1.0, far_part, 0.0))

def block_of(values, start_x, start_y, start_z, size_x, size_y, size_z):
    leading = values.shape[:-4]
    anchor = jnp.zeros((), jnp.int32)
    starts = (anchor,) * len(leading) + (start_x, start_y, start_z, anchor)
    return lax.dynamic_slice(values, starts, leading + (size_x, size_y, size_z, values.shape[-1]))

def flatten(values):
    return values.reshape(values.shape[:-4] + (-1, values.shape[-1]))

def offsets(number):
    number = jnp.asarray(number).astype(jnp.int32)
    return (number // 9, number // 3 % 3, number % 3)

def density_sum(targets, grid_pos, grid_weight, rows):
    size_x, size_y, size_z = (grid_pos.shape[1] - 2, grid_pos.shape[2] - 2, grid_pos.shape[3] - 2)
    picked = jnp.moveaxis(targets[:, :, :rows], 1, 0)

    def add_cells(number, running):
        step_x, step_y, step_z = offsets(number)
        source = jnp.moveaxis(flatten(block_of(grid_pos, step_x, step_y, step_z, size_x, size_y, size_z)), 1, 0)
        source_weight = flatten(block_of(grid_weight, step_x, step_y, step_z, size_x, size_y, size_z))
        displace = jnp.stack([step_x, step_y, step_z]).astype(jnp.float32) - 1.0

        def one_cell(items):
            own, far, far_weight = items
            between = own[:, :, None] - far[:, None, :] - displace[:, None, None]
            radius_sq = lax.optimization_barrier(jnp.sum(between * between, 0))
            return lax.optimization_barrier(jnp.sum(far_weight[None, :] * kernel_value(radius_sq), 1))
        return running + lax.map(one_cell, (picked, source, source_weight))
    return lax.fori_loop(0, 27, add_cells, jnp.zeros((picked.shape[0], picked.shape[2]), jnp.float32))

def force_sum(targets, margins, rows):
    own_pos, own_vel, own_rho, own_sound, own_press = [item[..., :rows] for item in targets]
    own_pos = jnp.moveaxis(own_pos, 1, 0)
    own_vel = jnp.moveaxis(own_vel, 1, 0)
    size_x, size_y, size_z = (margins[0].shape[1] - 2, margins[0].shape[2] - 2, margins[0].shape[3] - 2)

    def add_cells(number, running):
        step_x, step_y, step_z = offsets(number)
        pieces = [flatten(block_of(item, step_x, step_y, step_z, size_x, size_y, size_z)) for item in margins]
        far_pos, far_vel, far_weight, far_rho, far_sound, far_press = pieces
        far_pos = jnp.moveaxis(far_pos, 1, 0)
        far_vel = jnp.moveaxis(far_vel, 1, 0)
        displace = jnp.stack([step_x, step_y, step_z]).astype(jnp.float32) - 1.0

        def one_cell(items):
            mine_pos, mine_vel, mine_rho, mine_sound, mine_press, other_pos, other_vel, other_weight, other_rho, other_sound, other_press = items
            between = mine_pos[:, :, None] - other_pos[:, None, :] - displace[:, None, None]
            radius_sq = lax.optimization_barrier(jnp.sum(between * between, 0))
            closing = lax.optimization_barrier(jnp.sum((mine_vel[:, :, None] - other_vel[:, None, :]) * between, 0))
            approach = jnp.minimum(closing, 0.0) / (radius_sq + SOFTEN)
            mean_sound = 0.5 * (mine_sound[:, None] + other_sound[None, :])
            mean_rho = 0.5 * (mine_rho[:, None] + other_rho[None, :])
            viscous = (BETA * approach * approach - ALPHA * mean_sound * approach) / mean_rho
            factor = other_weight[None, :] * (mine_press[:, None] + other_press[None, :] + viscous) * kernel_slope(radius_sq)
            return lax.optimization_barrier(jnp.sum(factor[None] * between, 2))
        items = (own_pos, own_vel, own_rho, own_sound, own_press, far_pos, far_vel, far_weight, far_rho, far_sound, far_press)
        return running - lax.map(one_cell, items)
    total = lax.fori_loop(0, 27, add_cells, jnp.zeros(own_pos.shape, jnp.float32))
    return jnp.moveaxis(total, 0, 1)

def states_of(safe_density, entropy):
    pressure_term = entropy * safe_density ** (GAMMA - 2.0)
    sound_speed = jnp.sqrt(GAMMA * entropy * safe_density ** (GAMMA - 1.0))
    return (pressure_term, sound_speed)

def periodic(values):
    widths = [(0, 0)] * (values.ndim - 4) + [(1, 1)] * 3 + [(0, 0)]
    return jnp.pad(values, widths, mode='wrap')

def assemble(blocks):
    leading = blocks.shape[1:-2]
    lead_count = len(leading)
    shaped = blocks.reshape((N_GX, N_GY, N_GZ) + leading + (LX, LY, LZ, PC))
    reorder = tuple(range(3, 3 + lead_count)) + (0, 3 + lead_count, 1, 4 + lead_count, 2, 5 + lead_count, 6 + lead_count)
    return shaped.transpose(reorder).reshape(leading + (NX, NY, NZ, PC))

def corners(number):
    along_x = number // (N_GY * N_GZ)
    along_y = number // N_GZ % N_GY
    along_z = number % N_GZ
    return (along_x * LX, along_y * LY, along_z * LZ)

def reference(positions, velocities, masses, entropy, counts):
    slot_ids = lax.broadcasted_iota(jnp.int32, masses.shape, 3)
    active = slot_ids < counts[..., None]
    weight = jnp.where(active, masses, 0.0)
    wide_pos = periodic(positions)
    wide_weight = periodic(weight)
    numbers = jnp.arange(N_GX * N_GY * N_GZ, dtype=jnp.int32)

    def block_density(number):
        corner_x, corner_y, corner_z = corners(number)
        targets = flatten(block_of(positions, corner_x, corner_y, corner_z, LX, LY, LZ))
        grid_pos = block_of(wide_pos, corner_x, corner_y, corner_z, LX + 2, LY + 2, LZ + 2)
        grid_weight = block_of(wide_weight, corner_x, corner_y, corner_z, LX + 2, LY + 2, LZ + 2)
        return density_sum(targets, grid_pos, grid_weight, PC)
    raw_density = assemble(lax.map(block_density, numbers))
    safe_density = jnp.where(active, raw_density, 1.0)
    pressure_term, sound_speed = states_of(safe_density, entropy)
    owned = (positions, velocities, safe_density, sound_speed, pressure_term)
    widened = [periodic(item) for item in (positions, velocities, weight, safe_density, sound_speed, pressure_term)]

    def block_force(number):
        corner_x, corner_y, corner_z = corners(number)
        targets = tuple((flatten(block_of(item, corner_x, corner_y, corner_z, LX, LY, LZ)) for item in owned))
        margins = tuple((block_of(item, corner_x, corner_y, corner_z, LX + 2, LY + 2, LZ + 2) for item in widened))
        return force_sum(targets, margins, PC)
    raw_accel = assemble(lax.map(block_force, numbers))
    density = jnp.where(active, raw_density, 0.0)
    acceleration = jnp.where(active[None], raw_accel, 0.0)
    return (density, acceleration)
```

```python
import functools
import itertools
import math

import jax
import jax.numpy as jnp
import numpy as np
from jax import lax
from jax.experimental import pallas as pl
from jax.experimental.pallas import tpu as pltpu
from jax.sharding import PartitionSpec as P


SIGMA = 8.0 / math.pi
GAMMA = 5.0 / 3.0
SOFTEN = 0.01
TINY = 1e-24
LANES = 128
LANE_BITS = 7
ROWS = 64
CHUNKS = 2
SHARES = ((0, 1), (1, 2), (2, 8))
VMEM = pl.BlockSpec(memory_space=pltpu.VMEM)
SMEM = pl.BlockSpec(memory_space=pltpu.SMEM)
PARAMS = pltpu.CompilerParams(vmem_limit_bytes=24 << 20)


def shifted(size, step):
    return [(i, (i + step) % size) for i in range(size)]


def with_halo(block, sides):
    for axis, dim in sides:
        count = lax.axis_size(axis)
        size = block.shape[dim]
        if count == 2 and size == 2:
            other = lax.ppermute(block, axis, shifted(2, 1))
            low = lax.slice_in_dim(other, size - 1, None, axis=dim)
            high = lax.slice_in_dim(other, 0, 1, axis=dim)
        else:
            last = lax.slice_in_dim(block, size - 1, None, axis=dim)
            first = lax.slice_in_dim(block, 0, 1, axis=dim)
            low = lax.ppermute(last, axis, shifted(count, 1))
            high = lax.ppermute(first, axis, shifted(count, -1))
        if dim == sides[-1][1]:
            return [block, low, high]
        block = jnp.concatenate([low, block, high], axis=dim)


def halo_cells(sizes):
    wide = tuple(size + 2 for size in sizes)
    found = []
    for cell in itertools.product(*(range(size) for size in wide)):
        away = tuple(
            -1 if c == 0 else (1 if c == size + 1 else 0) for c, size in zip(cell, sizes)
        )
        if away == (0, 0, 0):
            continue
        index = (cell[0] * wide[1] + cell[1]) * wide[2] + cell[2]
        operand = {0: 0, -1: 1, 1: 2}[away[1]]
        within = cell[1] - 1 if away[1] == 0 else 0
        found.append((operand, (cell[0], within, cell[2]), index, away))
    return found


def halo_table(sizes):
    wide = tuple(size + 2 for size in sizes)
    table = []
    for own in itertools.product(*(range(size) for size in sizes)):
        line = []
        for step in itertools.product(range(3), repeat=3):
            cell = tuple(o + s for o, s in zip(own, step))
            if not all(1 <= c <= size for c, size in zip(cell, sizes)):
                line.append((cell[0] * wide[1] + cell[1]) * wide[2] + cell[2])
        table.append(line)
    assert all(len(line) == len(table[0]) for line in table)
    return np.array(table, np.int32)


def fill_list(cells, sources, lists, fills, group=CHUNKS):
    lane = lax.broadcasted_iota(jnp.int32, (8, LANES), 1)
    filled = jnp.int32(0)
    held = [jnp.full((8, LANES), fill, jnp.float32) for fill in fills]
    for cell, count in cells:
        base = lax.shift_right_logical(filled, LANE_BITS)
        shift = filled & (LANES - 1)
        keep = lane < shift
        filled = filled + count
        ahead = lax.shift_right_logical(filled, LANE_BITS) - base
        for number, (source, packed, fill) in enumerate(zip(sources, lists, fills)):
            slots = source.shape[-1]
            parts = [source[cell, :, pl.ds(at, LANES)] for at in range(0, slots, LANES)]
            parts = [pltpu.roll(part, shift, 1) for part in parts]
            edges = [held[number]] + parts + [fill]
            chunks = [jnp.where(keep, a, b) for a, b in zip(edges[:-1], edges[1:])]
            for at, chunk in enumerate(chunks):
                packed[base + at] = chunk
            held[number] = chunks[-1]
            for at in range(len(chunks) - 2, -1, -1):
                held[number] = jnp.where(ahead == at, chunks[at], held[number])
    end = lax.shift_right_logical(filled + LANES - 1, LANE_BITS)
    for packed, fill in zip(lists, fills):
        for at in range(group):
            packed[end + at] = jnp.full((8, LANES), fill, jnp.float32)
    return lax.div(end + group - 1, group)


def list_scratch(cells, slots):
    return pltpu.VMEM((cells * slots // LANES + 2 + CHUNKS, 8, LANES), jnp.float32)


def spread(tile, numbers, spread_ref, first=0):
    columns = jnp.transpose(tile)
    for at, n in enumerate(numbers):
        spread_ref[first + at] = jnp.broadcast_to(columns[:, n : n + 1], spread_ref.shape[1:])


def spread_chunk(tile, numbers, spread_ref, chunk, first=0):
    columns = jnp.transpose(tile)
    for at, n in enumerate(numbers):
        spread_ref[first + at, chunk] = jnp.broadcast_to(
            columns[:, n : n + 1], spread_ref.shape[2:]
        )


def lane_sums(values):
    return jnp.sum(jnp.transpose(values), axis=0, keepdims=True)


def separation(place, far):
    apart = [a - b for a, b in zip(place, far)]
    return apart, apart[0] * apart[0] + apart[1] * apart[1] + apart[2] * apart[2]


def kernel_value(radius_sq):
    radius_sq = jnp.maximum(radius_sq, TINY)
    outer = jnp.maximum(1.0 - radius_sq * lax.rsqrt(radius_sq), 0.0)
    twice = outer + outer
    inner = jnp.maximum(twice - 1.0, 0.0)
    return twice * outer * outer - inner * inner * inner


def pair_force(mine, far):
    apart, radius_sq = separation(mine[:3], far[:3])
    speed = [a - b for a, b in zip(mine[3:6], far[3:6])]
    closing = apart[0] * speed[0] + apart[1] * speed[1] + apart[2] * speed[2]
    closing = jnp.minimum(closing, 0.0)
    approach = closing / (radius_sq + SOFTEN)
    viscous = approach * (approach - (mine[7] + far[7])) / (mine[6] + far[6])
    radius_sq = jnp.maximum(radius_sq, TINY)
    inverse = lax.rsqrt(radius_sq)
    radius = radius_sq * inverse
    outer = jnp.maximum(1.0 - radius, 0.0)
    slope = jnp.where(radius < 0.5, 2.0 - 3.0 * radius, outer * outer * inverse)
    return slope * (mine[8] + far[8] + viscous), apart


def density_of(count, steps, list_ref, spread_ref, sum_ref):
    def one_group(group, carry):
        start = pl.multiple_of(group * ROWS, ROWS)

        def one_step(step, total):
            place = [spread_ref[n, pl.ds(start, ROWS), :] for n in range(3)]
            for at in range(CHUNKS):
                chunk = step * CHUNKS + at
                far = [list_ref[chunk, pl.ds(n, 1), :] for n in range(3)]
                weight = list_ref[chunk, pl.ds(6, 1), :]
                total = total + weight * kernel_value(separation(place, far)[1])
            return total

        total = lax.fori_loop(0, steps, one_step, jnp.zeros((ROWS, LANES), jnp.float32))
        sum_ref[pl.ds(start, ROWS), :] = total
        return carry

    lax.fori_loop(0, lax.div(count + ROWS - 1, ROWS), one_group, 0)
    slot = lax.broadcasted_iota(jnp.int32, (1, sum_ref.shape[0]), 1)
    return jnp.where(slot < count, SIGMA * lane_sums(sum_ref[...]), 0.0)


def force_of(count, steps, list_ref, state_list_ref, spread_ref, sum_ref):
    def one_group(group, carry):
        start = pl.multiple_of(group * ROWS, ROWS)

        def one_step(step, total):
            mine = [spread_ref[n, pl.ds(start, ROWS), :] for n in range(9)]
            for at in range(CHUNKS):
                chunk = step * CHUNKS + at
                far = [list_ref[chunk, pl.ds(n, 1), :] for n in range(6)]
                far += [state_list_ref[chunk, pl.ds(n, 1), :] for n in range(3)]
                factor, apart = pair_force(mine, far)
                factor = list_ref[chunk, pl.ds(6, 1), :] * factor
                total = tuple(t + factor * a for t, a in zip(total, apart))
            return total

        zero = jnp.zeros((ROWS, LANES), jnp.float32)
        total = lax.fori_loop(0, steps, one_step, (zero, zero, zero))
        for n in range(3):
            sum_ref[n, pl.ds(start, ROWS), :] = total[n]
        return carry

    lax.fori_loop(0, lax.div(count + ROWS - 1, ROWS), one_group, 0)
    slot = lax.broadcasted_iota(jnp.int32, (1, sum_ref.shape[1]), 1)
    return [
        jnp.where(slot < count, 6.0 * SIGMA * lane_sums(sum_ref[n]), 0.0) for n in range(3)
    ]


def folded(values):
    return jnp.sum(values.reshape(-1, 8, values.shape[-1]), axis=0)


def rows_of(chunks, share):
    first, last = share
    return lax.div(chunks * first + 7, 8), lax.div(chunks * last + 7, 8)


def pairs_within(chunks, rows, outputs, pair, sum_ref, fold_ref):
    span = fold_ref.shape[1]
    for n in range(outputs):
        fold_ref[n] = jnp.zeros(fold_ref.shape[1:], jnp.float32)

    def one_row(row, carry):
        def one_chunk(chunk, total):
            by_row, by_column = pair(row, chunk, True)
            for n in range(outputs):
                fold_ref[n, chunk] = fold_ref[n, chunk] + folded(by_column[n])
            return tuple(t + v for t, v in zip(total, by_row))

        total = lax.fori_loop(row + 1, chunks, one_chunk, tuple(pair(row, row, False)[0]))
        for n in range(outputs):
            sum_ref[n, row] = total[n]
        return carry

    lax.fori_loop(*rows, one_row, 0)

    def one_turn(number, carry):
        for at in range(2):
            row = rows[0] + number * 2 + at
            valid = row < rows[1]
            row = jnp.minimum(row, span - 1)
            for n in range(outputs):
                sums = folded(jnp.transpose(sum_ref[n, row]))
                fold_ref[n, row] = fold_ref[n, row] + jnp.where(valid, sums, 0.0)
        return carry

    lax.fori_loop(0, (rows[1] - rows[0] + 1) // 2, one_turn, 0)


def unpacked(fold_ref, number, filled, count, slots):
    lane = lax.broadcasted_iota(jnp.int32, (8, LANES), 1)
    base = lax.shift_right_logical(filled, LANE_BITS)
    back = LANES - (filled & (LANES - 1))
    turned = [
        pltpu.roll(fold_ref[number, base + at], back & (LANES - 1), 1) for at in range(slots // LANES + 1)
    ]
    parts = [jnp.where(lane < back, a, b) for a, b in zip(turned[:-1], turned[1:])]
    row = jnp.sum(jnp.concatenate(parts, axis=1), axis=0, keepdims=True)
    slot = lax.broadcasted_iota(jnp.int32, (1, slots), 1)
    return jnp.where(slot < count, row, 0.0)


def cell_place(target, sizes):
    target = jnp.asarray(target, jnp.int32)
    _, size_y, size_z = sizes
    along = lax.div(target, size_z)
    return lax.div(along, size_y), lax.rem(along, size_y), lax.rem(target, size_z)


def own_place(target, sizes):
    along_x, along_y, along_z = cell_place(target, sizes)
    return along_x, along_y, pl.ds(along_z, 1), slice(None)


def state_tile(density, entropy):
    density = jnp.broadcast_to(density, (8, density.shape[-1]))
    entropy = jnp.broadcast_to(entropy, (8, entropy.shape[-1]))
    active = entropy > 0.0
    safe = jnp.where(active, density, 1.0)
    third = jnp.exp(jnp.log(safe) * (1.0 / 3.0))
    sound = jnp.sqrt(GAMMA * entropy) * third
    row = lax.broadcasted_iota(jnp.int32, safe.shape, 0)
    tile = jnp.where(row == 0, 0.25 * safe, jnp.where(row == 1, 0.25 * sound, entropy / third))
    return tile


def pack_kernel(
    count_hbm, position_hbm, velocity_hbm, mass_hbm, entropy_hbm, out_ref,
    count_ref, position_ref, velocity_ref, mass_ref, entropy_ref, sems,
):
    sources = (count_hbm, position_hbm, velocity_hbm, mass_hbm, entropy_hbm)
    targets = (count_ref, position_ref, velocity_ref, mass_ref, entropy_ref)
    copies = [
        pltpu.make_async_copy(source, target, sems.at[n])
        for n, (source, target) in enumerate(zip(sources, targets))
    ]
    for copy in copies:
        copy.start()
    for copy in copies:
        copy.wait()
    slots = mass_ref.shape[-1]
    slot = lax.broadcasted_iota(jnp.int32, (8, slots), 1)
    for place in np.ndindex(mass_ref.shape[:3]):
        at = place[:2] + (pl.ds(place[2], 1), slice(None))
        rows = [position_ref[n, *at] + float(place[n]) for n in range(3)]
        rows += [velocity_ref[n, *at] for n in range(3)]
        rows += [mass_ref[at], entropy_ref[at]]
        tile = jnp.concatenate(rows, axis=0)
        out_ref[place] = jnp.where(slot < count_ref[place], tile, 0.0)


def density_own(count_ref, own_ref, out_ref, list_ref, spread_ref, sum_ref, fold_ref, *, share):
    _, _, slots = own_ref.shape
    counts = [count_ref[p] for p in np.ndindex(count_ref.shape)]
    chunks = fill_list(list(enumerate(counts)), [own_ref], [list_ref], [0.0], 1)

    def one_spread(chunk, carry):
        spread_chunk(list_ref[chunk], (0, 1, 2, 6), spread_ref, chunk)
        return carry

    rows = rows_of(chunks, share)
    lax.fori_loop(*rows, one_spread, 0)

    def pair(row, chunk, both):
        mine = [spread_ref[n, row] for n in range(4)]
        far = [list_ref[chunk, pl.ds(n, 1), :] for n in range(3)]
        value = kernel_value(separation(mine[:3], far)[1])
        weight = list_ref[chunk, pl.ds(6, 1), :]
        return [weight * value], [mine[3] * value] if both else None

    pairs_within(chunks, rows, 1, pair, sum_ref, fold_ref)
    filled = jnp.int32(0)
    for cell, count in enumerate(counts):
        out_ref[pl.ds(cell, 1), :] = SIGMA * unpacked(fold_ref, 0, filled, count, slots)
        filled = filled + count


def density_halo(
    count_ref, table_ref, own_ref, *refs, sizes, parts
):
    partial_refs, piece_refs = refs[:parts], refs[parts : parts + 3]
    rho_ref, again_ref, grid_ref, grid_count_ref, lists_ref, spread_ref, sum_ref = refs[
        parts + 3 :
    ]
    slots = own_ref.shape[-1]
    row = lax.broadcasted_iota(jnp.int32, (8, slots), 0)
    for operand, cell, index, away in halo_cells(sizes):
        tile = piece_refs[operand][cell[0], cell[1], cell[2]]
        grid_count_ref[index] = jnp.sum((tile[7:8] > 0.0).astype(jnp.int32))
        for dim in range(3):
            if away[dim]:
                tile = tile + jnp.where(row == dim, float(away[dim] * sizes[dim]), 0.0)
        grid_ref[index] = tile

    def one_target(target):
        cells = [table_ref[target, n] for n in range(table_ref.shape[1])]
        list_ref = lists_ref.at[target]
        steps = fill_list(
            [(c, grid_count_ref[c]) for c in cells], [grid_ref], [list_ref], [0.0]
        )
        spread(own_ref[target], range(3), spread_ref)
        return density_of(count_ref[*cell_place(target, sizes)], steps, list_ref, spread_ref, sum_ref)

    def one(target, carry):
        total = one_target(target)
        for partial_ref in partial_refs:
            total = total + partial_ref[pl.ds(target, 1), :]
        rho_ref[*own_place(target, sizes)] = total
        again_ref[*own_place(target, sizes)] = total
        return carry

    lax.fori_loop(0, own_ref.shape[0], one, 0)


def force_own(
    count_ref, own_ref, rho_ref, out_ref,
    list_ref, state_ref, state_list_ref, spread_ref, sum_ref, fold_ref, *, share,
):
    cells, _, slots = own_ref.shape
    counts = [count_ref[p] for p in np.ndindex(count_ref.shape)]
    for cell in range(cells):
        density = rho_ref[*own_place(cell, rho_ref.shape[:3])]
        state_ref[cell] = state_tile(density, own_ref[cell, pl.ds(7, 1), :])
    chunks = fill_list(
        list(enumerate(counts)), [own_ref, state_ref], [list_ref, state_list_ref], [0.0, 1.0], 1
    )

    def one_spread(chunk, carry):
        spread_chunk(list_ref[chunk], range(7), spread_ref, chunk)
        spread_chunk(state_list_ref[chunk], range(3), spread_ref, chunk, 7)
        return carry

    rows = rows_of(chunks, share)
    lax.fori_loop(*rows, one_spread, 0)

    def pair(row, chunk, both):
        mine = [spread_ref[n, row] for n in (0, 1, 2, 3, 4, 5, 7, 8, 9)]
        far = [list_ref[chunk, pl.ds(n, 1), :] for n in range(6)]
        far += [state_list_ref[chunk, pl.ds(n, 1), :] for n in range(3)]
        factor, apart = pair_force(mine, far)
        weight = list_ref[chunk, pl.ds(6, 1), :] * factor
        by_row = [weight * a for a in apart]
        if not both:
            return by_row, None
        weight = spread_ref[6, row] * factor
        return by_row, [-(weight * a) for a in apart]

    pairs_within(chunks, rows, 3, pair, sum_ref, fold_ref)
    for n in range(3):
        filled = jnp.int32(0)
        for cell, count in enumerate(counts):
            out_ref[n, pl.ds(cell, 1), :] = (6.0 * SIGMA) * unpacked(
                fold_ref, n, filled, count, slots
            )
            filled = filled + count


def force_halo(
    count_ref, table_ref, own_ref, density_ref, grid_count_ref, grid_ref, lists_ref,
    *refs, sizes, parts,
):
    partial_refs, piece_refs = refs[:parts], refs[parts : parts + 3]
    out_ref, state_ref, state_list_ref, spread_ref, sum_ref = refs[parts + 3 :]
    for operand, cell, index, _ in halo_cells(sizes):
        density = piece_refs[operand][cell[0], cell[1], pl.ds(cell[2], 1), :]
        state_ref[index] = state_tile(density, grid_ref[index, pl.ds(7, 1), :])

    def one_target(target):
        cells = [table_ref[target, n] for n in range(table_ref.shape[1])]
        steps = fill_list(
            [(c, grid_count_ref[c]) for c in cells], [state_ref], [state_list_ref], [1.0]
        )
        spread(own_ref[target], range(6), spread_ref)
        density = density_ref[*own_place(target, sizes)]
        spread(state_tile(density, own_ref[target, pl.ds(7, 1), :]), range(3), spread_ref, 6)
        return force_of(
            count_ref[*cell_place(target, sizes)], steps, lists_ref.at[target], state_list_ref, spread_ref, sum_ref
        )

    def one(target, carry):
        sums = one_target(target)
        for n in range(3):
            total = sums[n]
            for partial_ref in partial_refs:
                total = total + partial_ref[n, pl.ds(target, 1), :]
            out_ref[n, *own_place(target, sizes)] = total
        return carry

    lax.fori_loop(0, own_ref.shape[0], one, 0)


def cost(pairs, flops):
    return pl.CostEstimate(flops=pairs * flops, transcendentals=pairs, bytes_accessed=1 << 20)


def per_device(positions, velocities, masses, entropy, counts):
    sizes = masses.shape[:3]
    slots = masses.shape[3]
    cells = sizes[0] * sizes[1] * sizes[2]
    wide = (sizes[0] + 2) * (sizes[1] + 2) * (sizes[2] + 2)
    assert all(size <= 2 for size in sizes)
    packed = pl.pallas_call(
        pack_kernel,
        out_shape=jax.ShapeDtypeStruct(sizes + (8, slots), jnp.float32),
        in_specs=[pl.BlockSpec(memory_space=pltpu.HBM)] * 5,
        out_specs=VMEM,
        scratch_shapes=[
            pltpu.SMEM(counts.shape, jnp.int32),
            pltpu.VMEM(positions.shape, jnp.float32),
            pltpu.VMEM(velocities.shape, jnp.float32),
            pltpu.VMEM(masses.shape, jnp.float32),
            pltpu.VMEM(entropy.shape, jnp.float32),
            pltpu.SemaphoreType.DMA((5,)),
        ],
        compiler_params=PARAMS,
        name="pack",
    )(counts, positions, velocities, masses, entropy)
    own = packed.reshape(cells, 8, slots)
    table = jnp.asarray(halo_table(sizes))
    near = table.shape[1]
    pairs = cells * slots * slots
    own_chunks = cells * slots // LANES + 2

    def own_rows(fields):
        return pltpu.VMEM((fields, own_chunks, LANES, LANES), jnp.float32)

    def own_folds(outputs):
        return pltpu.VMEM((outputs, own_chunks, 8, LANES), jnp.float32)

    halo_order = (("gz", 2), ("gx", 0), ("gy", 1))
    spread3 = pltpu.VMEM((3, slots, LANES), jnp.float32)
    spread9 = pltpu.VMEM((9, slots, LANES), jnp.float32)
    sums = pltpu.VMEM((slots, LANES), jnp.float32)
    three_sums = pltpu.VMEM((3, slots, LANES), jnp.float32)
    own_list = list_scratch(cells, slots)
    halo_list = list_scratch(near, slots)

    partials = [pl.pallas_call(
        functools.partial(density_own, share=share),
        out_shape=jax.ShapeDtypeStruct((cells, slots), jnp.float32),
        in_specs=[SMEM, VMEM],
        out_specs=VMEM,
        scratch_shapes=[own_list, own_rows(4), own_rows(1), own_folds(1)],
        compiler_params=PARAMS,
        cost_estimate=cost(pairs * cells, 22),
    )(counts, own) for share in SHARES]
    pieces = with_halo(packed, halo_order)
    result, density, grid, grid_counts, lists = pl.pallas_call(
        functools.partial(density_halo, sizes=sizes, parts=len(SHARES)),
        out_shape=(
            jax.ShapeDtypeStruct(masses.shape, jnp.float32),
            jax.ShapeDtypeStruct(masses.shape, jnp.float32),
            jax.ShapeDtypeStruct((wide, 8, slots), jnp.float32),
            jax.ShapeDtypeStruct((wide,), jnp.int32),
            jax.ShapeDtypeStruct((cells,) + halo_list.shape, jnp.float32),
        ),
        in_specs=[SMEM, SMEM] + [VMEM] * (4 + len(SHARES)),
        out_specs=(VMEM, VMEM, VMEM, SMEM, VMEM),
        scratch_shapes=[spread3, sums],
        compiler_params=PARAMS,
        cost_estimate=cost(pairs * near, 22),
        name="density_halo",
    )(counts, table, own, *partials, *pieces)
    partials = [pl.pallas_call(
        functools.partial(force_own, share=share),
        out_shape=jax.ShapeDtypeStruct((3, cells, slots), jnp.float32),
        in_specs=[SMEM, VMEM, VMEM],
        out_specs=VMEM,
        scratch_shapes=[
            own_list, pltpu.VMEM((cells, 8, slots), jnp.float32), own_list,
            own_rows(10), own_rows(3), own_folds(3),
        ],
        compiler_params=PARAMS,
        cost_estimate=cost(pairs * cells, 50),
    )(counts, own, density) for share in SHARES]
    pieces = with_halo(density, halo_order)
    acceleration = pl.pallas_call(
        functools.partial(force_halo, sizes=sizes, parts=len(SHARES)),
        out_shape=jax.ShapeDtypeStruct(positions.shape, jnp.float32),
        in_specs=[SMEM, SMEM, VMEM, VMEM, SMEM] + [VMEM] * (5 + len(SHARES)),
        out_specs=VMEM,
        scratch_shapes=[
            pltpu.VMEM((wide, 8, slots), jnp.float32), halo_list,
            spread9, three_sums,
        ],
        compiler_params=PARAMS,
        cost_estimate=cost(pairs * near, 50),
        name="force_halo",
    )(counts, table, own, density, grid_counts, grid, lists, *partials, *pieces)
    return (result, acceleration)


def solution(mesh):
    return jax.shard_map(
        per_device,
        mesh=mesh,
        in_specs=(
            P(None, "gx", "gy", "gz", None),
            P(None, "gx", "gy", "gz", None),
            P("gx", "gy", "gz", None),
            P("gx", "gy", "gz", None),
            P("gx", "gy", "gz"),
        ),
        out_specs=(P("gx", "gy", "gz", None), P(None, "gx", "gy", "gz", None)),
        check_vma=False,
    )
```

```python
import functools
import itertools
import math

import jax
import jax.numpy as jnp
import numpy as np
from jax import lax
from jax.experimental import pallas as pl
from jax.experimental.pallas import tpu as pltpu
from jax.sharding import PartitionSpec as P


SIGMA = 8.0 / math.pi
GAMMA = 5.0 / 3.0
SOFTEN = 0.01
TINY = 1e-24
LANES = 128
LANE_BITS = 7
ROWS = 64
CHUNKS = 2
PAD = 8
PARTS = 16
ORDER = (("gy", 1), ("gz", 2), ("gx", 0))
DENSITY_SHARES = ((0, 3), (3, 6), (6, PARTS))
FORCE_SHARES = ((0, 2), (2, 4), (4, PARTS))
VMEM = pl.BlockSpec(memory_space=pltpu.VMEM)
SMEM = pl.BlockSpec(memory_space=pltpu.SMEM)
PARAMS = pltpu.CompilerParams(vmem_limit_bytes=24 << 20)


def shifted(size, step):
    return [(i, (i + step) % size) for i in range(size)]


def with_halo(block, sides):
    for axis, dim in sides:
        count = lax.axis_size(axis)
        size = block.shape[dim]
        if count == 2 and size == 2:
            other = lax.ppermute(block, axis, shifted(2, 1))
            low = lax.slice_in_dim(other, size - 1, None, axis=dim)
            high = lax.slice_in_dim(other, 0, 1, axis=dim)
        else:
            last = lax.slice_in_dim(block, size - 1, None, axis=dim)
            first = lax.slice_in_dim(block, 0, 1, axis=dim)
            low = lax.ppermute(last, axis, shifted(count, 1))
            high = lax.ppermute(first, axis, shifted(count, -1))
        if dim == sides[-1][1]:
            return [block, low, high]
        block = jnp.concatenate([low, block, high], axis=dim)


def halo_cells(sizes):
    wide = tuple(size + 2 for size in sizes)
    found = []
    for cell in itertools.product(*(range(size) for size in wide)):
        away = tuple(
            -1 if c == 0 else (1 if c == size + 1 else 0) for c, size in zip(cell, sizes)
        )
        if away == (0, 0, 0):
            continue
        index = (cell[0] * wide[1] + cell[1]) * wide[2] + cell[2]
        last = ORDER[-1][1]
        within = list(cell)
        within[last] = cell[last] - 1 if away[last] == 0 else 0
        found.append(({0: 0, -1: 1, 1: 2}[away[last]], tuple(within), index, away))
    return found


def halo_table(sizes):
    wide = tuple(size + 2 for size in sizes)
    table = []
    for own in itertools.product(*(range(size) for size in sizes)):
        line = []
        for step in itertools.product(range(3), repeat=3):
            cell = tuple(o + s for o, s in zip(own, step))
            if not all(1 <= c <= size for c, size in zip(cell, sizes)):
                line.append((cell[0] * wide[1] + cell[1]) * wide[2] + cell[2])
        table.append(line)
    assert all(len(line) == len(table[0]) for line in table)
    return np.array(table, np.int32)


def fill_list(cells, sources, lists, fills, group=CHUNKS):
    lane = lax.broadcasted_iota(jnp.int32, (8, LANES), 1)
    filled = jnp.int32(0)
    held = [jnp.full((8, LANES), fill, jnp.float32) for fill in fills]
    for cell, count in cells:
        base = lax.shift_right_logical(filled, LANE_BITS)
        shift = filled & (LANES - 1)
        keep = lane < shift
        filled = filled + count
        ahead = lax.shift_right_logical(filled, LANE_BITS) - base
        for number, (source, packed, fill) in enumerate(zip(sources, lists, fills)):
            slots = source.shape[-1]
            parts = [source[cell, :, pl.ds(at, LANES)] for at in range(0, slots, LANES)]
            parts = [pltpu.roll(part, shift, 1) for part in parts]
            edges = [held[number]] + parts + [fill]
            chunks = [jnp.where(keep, a, b) for a, b in zip(edges[:-1], edges[1:])]
            for at, chunk in enumerate(chunks):
                packed[base + at] = chunk
            held[number] = chunks[-1]
            for at in range(len(chunks) - 2, -1, -1):
                held[number] = jnp.where(ahead == at, chunks[at], held[number])
    end = lax.shift_right_logical(filled + LANES - 1, LANE_BITS)
    for packed, fill in zip(lists, fills):
        for at in range(group):
            packed[end + at] = jnp.full((8, LANES), fill, jnp.float32)
    return lax.div(end + group - 1, group)


def list_scratch(cells, slots):
    return pltpu.VMEM((cells * slots // LANES + 2 + CHUNKS, 8, LANES), jnp.float32)


def spread(tile, numbers, spread_ref, first=0):
    columns = jnp.transpose(tile)
    rows = columns.shape[0]
    for at, n in enumerate(numbers):
        spread_ref[first + at, pl.ds(0, rows), :] = jnp.broadcast_to(
            columns[:, n : n + 1], (rows, LANES)
        )


def rows_at(chunk):
    return pl.ds(pl.multiple_of(chunk * LANES, LANES), LANES)


def spread_chunk(tile, numbers, spread_ref, chunk, first=0):
    columns = jnp.transpose(tile)
    for at, n in enumerate(numbers):
        spread_ref[first + at, rows_at(chunk), :] = jnp.broadcast_to(
            columns[:, n : n + 1], (LANES, LANES)
        )


def in_twos(rows, work):
    first, last = rows

    def two(number, carry):
        row = first + 2 * number
        work(row)
        work(jnp.minimum(row + 1, last - 1))
        return carry

    lax.fori_loop(0, lax.div(last - first + 1, 2), two, 0)


def lane_sums(values):
    return jnp.sum(jnp.transpose(values), axis=0, keepdims=True)


def separation(place, far):
    apart = [a - b for a, b in zip(place, far)]
    return apart, apart[0] * apart[0] + apart[1] * apart[1] + apart[2] * apart[2]


def kernel_value(radius_sq):
    radius_sq = jnp.maximum(radius_sq, TINY)
    outer = jnp.maximum(1.0 - radius_sq * lax.rsqrt(radius_sq), 0.0)
    twice = outer + outer
    inner = jnp.maximum(twice - 1.0, 0.0)
    return twice * outer * outer - inner * inner * inner


def pair_force(mine, far):
    apart, radius_sq = separation(mine[:3], far[:3])
    speed = [a - b for a, b in zip(mine[3:6], far[3:6])]
    closing = apart[0] * speed[0] + apart[1] * speed[1] + apart[2] * speed[2]
    closing = jnp.minimum(closing, 0.0)
    approach = closing / (radius_sq + SOFTEN)
    viscous = approach * (approach - (mine[7] + far[7])) / (mine[6] + far[6])
    radius_sq = jnp.maximum(radius_sq, TINY)
    inverse = lax.rsqrt(radius_sq)
    radius = radius_sq * inverse
    outer = jnp.maximum(1.0 - radius, 0.0)
    slope = jnp.where(radius < 0.5, 2.0 - 3.0 * radius, outer * outer * inverse)
    return slope * (mine[8] + far[8] + viscous), apart


def density_of(count, steps, list_ref, spread_ref, sum_ref):
    def one_group(group, carry):
        start = pl.multiple_of(group * ROWS, ROWS)
        place = [spread_ref[n, pl.ds(start, ROWS), :] for n in range(3)]

        def one_step(step, total):
            for at in range(CHUNKS):
                chunk = step * CHUNKS + at
                far = [list_ref[chunk, pl.ds(n, 1), :] for n in range(3)]
                weight = list_ref[chunk, pl.ds(6, 1), :]
                total = total + weight * kernel_value(separation(place, far)[1])
            return total

        total = lax.fori_loop(0, steps, one_step, jnp.zeros((ROWS, LANES), jnp.float32))
        sum_ref[pl.ds(start, ROWS), :] = total
        return carry

    lax.fori_loop(0, lax.div(count + ROWS - 1, ROWS), one_group, 0)
    slot = lax.broadcasted_iota(jnp.int32, (1, sum_ref.shape[0]), 1)
    return jnp.where(slot < count, SIGMA * lane_sums(sum_ref[...]), 0.0)


def force_of(count, steps, list_ref, state_list_ref, spread_ref, sum_ref):
    def one_group(group, carry):
        start = pl.multiple_of(group * ROWS, ROWS)

        def one_step(step, total):
            mine = [spread_ref[n, pl.ds(start, ROWS), :] for n in range(9)]
            for at in range(CHUNKS):
                chunk = step * CHUNKS + at
                far = [list_ref[chunk, pl.ds(n, 1), :] for n in range(6)]
                far += [state_list_ref[chunk, pl.ds(n, 1), :] for n in range(3)]
                factor, apart = pair_force(mine, far)
                factor = list_ref[chunk, pl.ds(6, 1), :] * factor
                total = tuple(t + factor * a for t, a in zip(total, apart))
            return total

        zero = jnp.zeros((ROWS, LANES), jnp.float32)
        total = lax.fori_loop(0, steps, one_step, (zero, zero, zero))
        for n in range(3):
            sum_ref[n, pl.ds(start, ROWS), :] = total[n]
        return carry

    lax.fori_loop(0, lax.div(count + ROWS - 1, ROWS), one_group, 0)
    slot = lax.broadcasted_iota(jnp.int32, (1, sum_ref.shape[1]), 1)
    return [
        jnp.where(slot < count, 6.0 * SIGMA * lane_sums(sum_ref[n]), 0.0) for n in range(3)
    ]


def folded(values):
    return jnp.sum(values.reshape(-1, 8, values.shape[-1]), axis=0)


def rows_of(chunks, share):
    first, last = share
    return tuple(lax.div(chunks * end + PARTS - 1, PARTS) for end in (first, last))


def pairs_within(chunks, rows, outputs, pair, sum_ref, fold_ref):
    span = fold_ref.shape[1]
    for n in range(outputs):
        fold_ref[n] = jnp.zeros(fold_ref.shape[1:], jnp.float32)

    def one_row(row, carry):
        def one_chunk(chunk, total):
            by_row, by_column = pair(row, chunk, True)
            for n in range(outputs):
                fold_ref[n, chunk] = fold_ref[n, chunk] + folded(by_column[n])
            return tuple(t + v for t, v in zip(total, by_row))

        total = lax.fori_loop(row + 1, chunks, one_chunk, tuple(pair(row, row, False)[0]))
        for n in range(outputs):
            sum_ref[n, row] = total[n]
        return carry

    lax.fori_loop(*rows, one_row, 0)

    def one_turn(number, carry):
        for at in range(2):
            row = rows[0] + number * 2 + at
            valid = row < rows[1]
            row = jnp.minimum(row, span - 1)
            for n in range(outputs):
                sums = folded(jnp.transpose(sum_ref[n, row]))
                fold_ref[n, row] = fold_ref[n, row] + jnp.where(valid, sums, 0.0)
        return carry

    lax.fori_loop(0, (rows[1] - rows[0] + 1) // 2, one_turn, 0)


def unpacked(fold_ref, number, filled, count, slots):
    lane = lax.broadcasted_iota(jnp.int32, (8, LANES), 1)
    base = lax.shift_right_logical(filled, LANE_BITS)
    back = LANES - (filled & (LANES - 1))
    turned = [
        pltpu.roll(fold_ref[number, base + at], back & (LANES - 1), 1) for at in range(slots // LANES + 1)
    ]
    parts = [jnp.where(lane < back, a, b) for a, b in zip(turned[:-1], turned[1:])]
    row = jnp.sum(jnp.concatenate(parts, axis=1), axis=0, keepdims=True)
    slot = lax.broadcasted_iota(jnp.int32, (1, slots), 1)
    return jnp.where(slot < count, row, 0.0)


def cell_place(target, sizes):
    target = jnp.asarray(target, jnp.int32)
    _, size_y, size_z = sizes
    along = lax.div(target, size_z)
    return lax.div(along, size_y), lax.rem(along, size_y), lax.rem(target, size_z)


def own_place(target, sizes):
    along_x, along_y, along_z = cell_place(target, sizes)
    return along_x, along_y, pl.ds(along_z, 1), slice(None)


def state_tile(density, entropy):
    density = jnp.broadcast_to(density, (8, density.shape[-1]))
    entropy = jnp.broadcast_to(entropy, (8, entropy.shape[-1]))
    active = entropy > 0.0
    safe = jnp.where(active, density, 1.0)
    third = jnp.exp(jnp.log(safe) * (1.0 / 3.0))
    sound = jnp.sqrt(GAMMA * entropy) * third
    row = lax.broadcasted_iota(jnp.int32, safe.shape, 0)
    tile = jnp.where(row == 0, 0.25 * safe, jnp.where(row == 1, 0.25 * sound, entropy / third))
    return tile


def pack_kernel(
    count_hbm, position_hbm, velocity_hbm, mass_hbm, entropy_hbm, out_ref, count_out,
    count_ref, position_ref, velocity_ref, mass_ref, entropy_ref, sems,
):
    sources = (count_hbm, position_hbm, velocity_hbm, mass_hbm, entropy_hbm)
    targets = (count_ref, position_ref, velocity_ref, mass_ref, entropy_ref)
    copies = [
        pltpu.make_async_copy(source, target, sems.at[n])
        for n, (source, target) in enumerate(zip(sources, targets))
    ]
    for copy in copies:
        copy.start()
    for copy in copies:
        copy.wait()
    slots = mass_ref.shape[-1]
    slot = lax.broadcasted_iota(jnp.int32, (8, slots), 1)
    for cell, place in enumerate(np.ndindex(mass_ref.shape[:3])):
        count_out[cell] = count_ref[place]
        at = place[:2] + (pl.ds(place[2], 1), slice(None))
        rows = [position_ref[n, *at] + float(place[n]) for n in range(3)]
        rows += [velocity_ref[n, *at] for n in range(3)]
        rows += [mass_ref[at], entropy_ref[at]]
        tile = jnp.concatenate(rows, axis=0)
        out_ref[place] = jnp.where(slot < count_ref[place], tile, 0.0)


def density_own(count_ref, own_ref, out_ref, list_ref, spread_ref, sum_ref, fold_ref, *, share):
    cells, _, slots = own_ref.shape
    counts = [count_ref[c] for c in range(cells)]
    chunks = fill_list(list(enumerate(counts)), [own_ref], [list_ref], [0.0], 1)

    rows = rows_of(chunks, share)

    def one_spread(chunk):
        spread_chunk(list_ref[chunk], (0, 1, 2, 6), spread_ref, chunk)

    in_twos(rows, one_spread)

    def pair(row, chunk, both):
        mine = [spread_ref[n, rows_at(row), :] for n in range(4)]
        far = [list_ref[chunk, pl.ds(n, 1), :] for n in range(3)]
        value = kernel_value(separation(mine[:3], far)[1])
        weight = list_ref[chunk, pl.ds(6, 1), :]
        return [weight * value], [mine[3] * value] if both else None

    pairs_within(chunks, rows, 1, pair, sum_ref, fold_ref)
    filled = jnp.int32(0)
    for cell, count in enumerate(counts):
        out_ref[pl.ds(cell, 1), :] = SIGMA * unpacked(fold_ref, 0, filled, count, slots)
        filled = filled + count


def density_halo(
    count_ref, table_ref, own_ref, *refs, sizes, parts
):
    partial_refs, piece_refs = refs[:parts], refs[parts : parts + 3]
    rho_ref, again_ref, grid_ref, grid_count_ref, lists_ref, spread_ref, sum_ref = refs[
        parts + 3 :
    ]
    slots = own_ref.shape[-1]
    row = lax.broadcasted_iota(jnp.int32, (8, slots), 0)
    for operand, cell, index, away in halo_cells(sizes):
        tile = piece_refs[operand][cell[0], cell[1], cell[2]]
        grid_count_ref[index] = jnp.sum((tile[7:8] > 0.0).astype(jnp.int32))
        for dim in range(3):
            if away[dim]:
                tile = tile + jnp.where(row == dim, float(away[dim] * sizes[dim]), 0.0)
        grid_ref[index] = tile

    def one_target(target):
        cells = [table_ref[target, n] for n in range(table_ref.shape[1])]
        list_ref = lists_ref.at[target]
        steps = fill_list(
            [(c, grid_count_ref[c]) for c in cells], [grid_ref], [list_ref], [0.0]
        )
        spread(own_ref[target], range(3), spread_ref)
        return density_of(count_ref[target], steps, list_ref, spread_ref, sum_ref)

    def one(target, carry):
        total = one_target(target)
        for partial_ref in partial_refs:
            total = total + partial_ref[pl.ds(target, 1), :]
        rho_ref[*own_place(target, sizes)] = total
        again_ref[*own_place(target, sizes)] = total
        return carry

    lax.fori_loop(0, own_ref.shape[0], one, 0)


def force_own(
    count_ref, own_ref, rho_ref, out_ref,
    list_ref, state_ref, state_list_ref, spread_ref, sum_ref, fold_ref, *, share,
):
    cells, _, slots = own_ref.shape
    counts = [count_ref[c] for c in range(cells)]
    for cell in range(cells):
        density = rho_ref[*own_place(cell, rho_ref.shape[:3])]
        state_ref[cell] = state_tile(density, own_ref[cell, pl.ds(7, 1), :])
    chunks = fill_list(
        list(enumerate(counts)), [own_ref, state_ref], [list_ref, state_list_ref], [0.0, 1.0], 1
    )

    rows = rows_of(chunks, share)

    def one_spread(chunk):
        spread_chunk(list_ref[chunk], range(7), spread_ref, chunk)
        spread_chunk(state_list_ref[chunk], range(3), spread_ref, chunk, 7)

    in_twos(rows, one_spread)

    def pair(row, chunk, both):
        mine = [spread_ref[n, rows_at(row), :] for n in (0, 1, 2, 3, 4, 5, 7, 8, 9)]
        far = [list_ref[chunk, pl.ds(n, 1), :] for n in range(6)]
        far += [state_list_ref[chunk, pl.ds(n, 1), :] for n in range(3)]
        factor, apart = pair_force(mine, far)
        weight = list_ref[chunk, pl.ds(6, 1), :] * factor
        by_row = [weight * a for a in apart]
        if not both:
            return by_row, None
        weight = spread_ref[6, rows_at(row), :] * factor
        return by_row, [-(weight * a) for a in apart]

    pairs_within(chunks, rows, 3, pair, sum_ref, fold_ref)
    for n in range(3):
        filled = jnp.int32(0)
        for cell, count in enumerate(counts):
            out_ref[n, pl.ds(cell, 1), :] = (6.0 * SIGMA) * unpacked(
                fold_ref, n, filled, count, slots
            )
            filled = filled + count


def force_halo(
    count_ref, table_ref, own_ref, density_ref, grid_count_ref, grid_ref, lists_ref,
    *refs, sizes, parts,
):
    partial_refs, piece_refs = refs[:parts], refs[parts : parts + 3]
    out_ref, state_ref, state_list_ref, spread_ref, sum_ref = refs[parts + 3 :]
    for operand, cell, index, _ in halo_cells(sizes):
        density = piece_refs[operand][cell[0], cell[1], pl.ds(cell[2], 1), :]
        state_ref[index] = state_tile(density, grid_ref[index, pl.ds(7, 1), :])

    def one_target(target):
        cells = [table_ref[target, n] for n in range(table_ref.shape[1])]
        steps = fill_list(
            [(c, grid_count_ref[c]) for c in cells], [state_ref], [state_list_ref], [1.0]
        )
        spread(own_ref[target], range(6), spread_ref)
        density = density_ref[*own_place(target, sizes)]
        spread(state_tile(density, own_ref[target, pl.ds(7, 1), :]), range(3), spread_ref, 6)
        return force_of(
            count_ref[target], steps, lists_ref.at[target], state_list_ref, spread_ref, sum_ref
        )

    def one(target, carry):
        sums = one_target(target)
        for n in range(3):
            total = sums[n]
            for partial_ref in partial_refs:
                total = total + partial_ref[n, pl.ds(target, 1), :]
            out_ref[n, *own_place(target, sizes)] = total
        return carry

    lax.fori_loop(0, own_ref.shape[0], one, 0)


def cost(pairs, flops):
    return pl.CostEstimate(flops=pairs * flops, transcendentals=pairs, bytes_accessed=1 << 20)


def per_device(positions, velocities, masses, entropy, counts):
    sizes = masses.shape[:3]
    slots = masses.shape[3]
    cells = sizes[0] * sizes[1] * sizes[2]
    wide = (sizes[0] + 2) * (sizes[1] + 2) * (sizes[2] + 2)
    assert all(size <= 2 for size in sizes)
    packed, own_counts = pl.pallas_call(
        pack_kernel,
        out_shape=(
            jax.ShapeDtypeStruct(sizes + (8, slots), jnp.float32),
            jax.ShapeDtypeStruct((cells,), jnp.int32),
        ),
        in_specs=[pl.BlockSpec(memory_space=pltpu.HBM)] * 5,
        out_specs=(VMEM, SMEM),
        scratch_shapes=[
            pltpu.SMEM(counts.shape, jnp.int32),
            pltpu.VMEM(positions.shape, jnp.float32),
            pltpu.VMEM(velocities.shape, jnp.float32),
            pltpu.VMEM(masses.shape, jnp.float32),
            pltpu.VMEM(entropy.shape, jnp.float32),
            pltpu.SemaphoreType.DMA((5,)),
        ],
        compiler_params=PARAMS,
        name="pack",
    )(
        *(
            pltpu.with_memory_space_constraint(item, pltpu.HBM)
            for item in (counts, positions, velocities, masses, entropy)
        )
    )
    own = packed.reshape(cells, 8, slots)
    table = jnp.asarray(halo_table(sizes))
    near = table.shape[1]
    pairs = cells * slots * slots
    own_chunks = cells * slots // LANES + 2

    def own_rows(fields):
        return pltpu.VMEM((fields, own_chunks, LANES, LANES), jnp.float32)

    def own_spread(fields):
        return pltpu.VMEM((fields, own_chunks * LANES + PAD, LANES), jnp.float32)

    def own_folds(outputs):
        return pltpu.VMEM((outputs, own_chunks, 8, LANES), jnp.float32)

    spread3 = pltpu.VMEM((3, slots + PAD, LANES), jnp.float32)
    spread9 = pltpu.VMEM((9, slots + PAD, LANES), jnp.float32)
    sums = pltpu.VMEM((slots, LANES), jnp.float32)
    three_sums = pltpu.VMEM((3, slots, LANES), jnp.float32)
    own_list = list_scratch(cells, slots)
    halo_list = list_scratch(near, slots)

    partials = [pl.pallas_call(
        functools.partial(density_own, share=share),
        out_shape=jax.ShapeDtypeStruct((cells, slots), jnp.float32),
        in_specs=[SMEM, VMEM],
        out_specs=VMEM,
        scratch_shapes=[own_list, own_spread(4), own_rows(1), own_folds(1)],
        compiler_params=PARAMS,
        cost_estimate=cost(pairs * cells, 22),
    )(own_counts, own) for share in DENSITY_SHARES]
    pieces = with_halo(packed, ORDER)
    result, density, grid, grid_counts, lists = pl.pallas_call(
        functools.partial(density_halo, sizes=sizes, parts=len(DENSITY_SHARES)),
        out_shape=(
            jax.ShapeDtypeStruct(masses.shape, jnp.float32),
            jax.ShapeDtypeStruct(masses.shape, jnp.float32),
            jax.ShapeDtypeStruct((wide, 8, slots), jnp.float32),
            jax.ShapeDtypeStruct((wide,), jnp.int32),
            jax.ShapeDtypeStruct((cells,) + halo_list.shape, jnp.float32),
        ),
        in_specs=[SMEM, SMEM] + [VMEM] * (4 + len(DENSITY_SHARES)),
        out_specs=(VMEM, VMEM, VMEM, SMEM, VMEM),
        scratch_shapes=[spread3, sums],
        compiler_params=PARAMS,
        cost_estimate=cost(pairs * near, 22),
        name="density_halo",
    )(own_counts, table, own, *partials, *pieces)
    partials = [pl.pallas_call(
        functools.partial(force_own, share=share),
        out_shape=jax.ShapeDtypeStruct((3, cells, slots), jnp.float32),
        in_specs=[SMEM, VMEM, VMEM],
        out_specs=VMEM,
        scratch_shapes=[
            own_list, pltpu.VMEM((cells, 8, slots), jnp.float32), own_list,
            own_spread(10), own_rows(3), own_folds(3),
        ],
        compiler_params=PARAMS,
        cost_estimate=cost(pairs * cells, 50),
    )(own_counts, own, density) for share in FORCE_SHARES]
    pieces = with_halo(density, ORDER)
    acceleration = pl.pallas_call(
        functools.partial(force_halo, sizes=sizes, parts=len(FORCE_SHARES)),
        out_shape=jax.ShapeDtypeStruct(positions.shape, jnp.float32),
        in_specs=[SMEM, SMEM, VMEM, VMEM, SMEM] + [VMEM] * (5 + len(FORCE_SHARES)),
        out_specs=VMEM,
        scratch_shapes=[
            pltpu.VMEM((wide, 8, slots), jnp.float32), halo_list,
            spread9, three_sums,
        ],
        compiler_params=PARAMS,
        cost_estimate=cost(pairs * near, 50),
        name="force_halo",
    )(own_counts, table, own, density, grid_counts, grid, lists, *partials, *pieces)
    return (result, acceleration)


def solution(mesh):
    return jax.shard_map(
        per_device,
        mesh=mesh,
        in_specs=(
            P(None, "gx", "gy", "gz", None),
            P(None, "gx", "gy", "gz", None),
            P("gx", "gy", "gz", None),
            P("gx", "gy", "gz", None),
            P("gx", "gy", "gz"),
        ),
        out_specs=(P("gx", "gy", "gz", None), P(None, "gx", "gy", "gz", None)),
        check_vma=False,
    )
```

```python
import functools
import itertools
import math

import jax
import jax.numpy as jnp
import numpy as np
from jax import lax
from jax.experimental import pallas as pl
from jax.experimental.pallas import tpu as pltpu
from jax.sharding import PartitionSpec as P


SIGMA = 8.0 / math.pi
GAMMA = 5.0 / 3.0
SOFTEN = 0.01
TINY = 1e-24
LANES = 128
LANE_BITS = 7
ROWS = 64
CHUNKS = 2
PAD = 8
PARTS = 16
ORDER = (("gy", 1), ("gz", 2), ("gx", 0))
DENSITY_SHARES = ((0, 3), (3, 6), (6, PARTS))
FORCE_SHARES = ((0, 2), (2, 4), (4, PARTS))
VMEM = pl.BlockSpec(memory_space=pltpu.VMEM)
SMEM = pl.BlockSpec(memory_space=pltpu.SMEM)
PARAMS = pltpu.CompilerParams(vmem_limit_bytes=24 << 20)
DENSITY_PARAMS = pltpu.CompilerParams(vmem_limit_bytes=24 << 20)


def shifted(size, step):
    return [(i, (i + step) % size) for i in range(size)]


def with_halo(block, sides):
    for axis, dim in sides:
        count = lax.axis_size(axis)
        size = block.shape[dim]
        if count == 2 and size == 2:
            other = lax.ppermute(block, axis, shifted(2, 1))
            low = lax.slice_in_dim(other, size - 1, None, axis=dim)
            high = lax.slice_in_dim(other, 0, 1, axis=dim)
        else:
            last = lax.slice_in_dim(block, size - 1, None, axis=dim)
            first = lax.slice_in_dim(block, 0, 1, axis=dim)
            low = lax.ppermute(last, axis, shifted(count, 1))
            high = lax.ppermute(first, axis, shifted(count, -1))
        if dim == sides[-1][1]:
            return [block, low, high]
        block = jnp.concatenate([low, block, high], axis=dim)


def halo_cells(sizes):
    wide = tuple(size + 2 for size in sizes)
    found = []
    for cell in itertools.product(*(range(size) for size in wide)):
        away = tuple(
            -1 if c == 0 else (1 if c == size + 1 else 0) for c, size in zip(cell, sizes)
        )
        if away == (0, 0, 0):
            continue
        index = (cell[0] * wide[1] + cell[1]) * wide[2] + cell[2]
        last = ORDER[-1][1]
        within = list(cell)
        within[last] = cell[last] - 1 if away[last] == 0 else 0
        found.append(({0: 0, -1: 1, 1: 2}[away[last]], tuple(within), index, away))
    return found


def halo_table(sizes):
    wide = tuple(size + 2 for size in sizes)
    table = []
    for own in itertools.product(*(range(size) for size in sizes)):
        line = []
        for step in itertools.product(range(3), repeat=3):
            cell = tuple(o + s for o, s in zip(own, step))
            if not all(1 <= c <= size for c, size in zip(cell, sizes)):
                line.append((cell[0] * wide[1] + cell[1]) * wide[2] + cell[2])
        table.append(line)
    assert all(len(line) == len(table[0]) for line in table)
    return np.array(table, np.int32)


def fill_list(cells, sources, lists, fills, group=CHUNKS):
    lane = lax.broadcasted_iota(jnp.int32, (8, LANES), 1)
    filled = jnp.int32(0)
    held = [jnp.full((8, LANES), fill, jnp.float32) for fill in fills]
    for cell, count in cells:
        base = lax.shift_right_logical(filled, LANE_BITS)
        shift = filled & (LANES - 1)
        keep = lane < shift
        filled = filled + count
        ahead = lax.shift_right_logical(filled, LANE_BITS) - base
        for number, (source, packed, fill) in enumerate(zip(sources, lists, fills)):
            slots = source.shape[-1]
            parts = [source[cell, :, pl.ds(at, LANES)] for at in range(0, slots, LANES)]
            parts = [pltpu.roll(part, shift, 1) for part in parts]
            edges = [held[number]] + parts + [fill]
            chunks = [jnp.where(keep, a, b) for a, b in zip(edges[:-1], edges[1:])]
            for at, chunk in enumerate(chunks):
                packed[base + at] = chunk
            held[number] = chunks[-1]
            for at in range(len(chunks) - 2, -1, -1):
                held[number] = jnp.where(ahead == at, chunks[at], held[number])
    end = lax.shift_right_logical(filled + LANES - 1, LANE_BITS)
    for packed, fill in zip(lists, fills):
        for at in range(group):
            packed[end + at] = jnp.full((8, LANES), fill, jnp.float32)
    return lax.div(end + group - 1, group)


def list_scratch(cells, slots):
    return pltpu.VMEM((cells * slots // LANES + 2 + CHUNKS, 8, LANES), jnp.float32)


def spread(tile, numbers, spread_ref, first=0):
    columns = jnp.transpose(tile)
    rows = columns.shape[0]
    for at, n in enumerate(numbers):
        spread_ref[first + at, pl.ds(0, rows), :] = jnp.broadcast_to(
            columns[:, n : n + 1], (rows, LANES)
        )


def rows_at(chunk):
    return pl.ds(pl.multiple_of(chunk * LANES, LANES), LANES)


def spread_chunk(tile, numbers, spread_ref, chunk, first=0):
    columns = jnp.transpose(tile)
    for at, n in enumerate(numbers):
        spread_ref[first + at, rows_at(chunk), :] = jnp.broadcast_to(
            columns[:, n : n + 1], (LANES, LANES)
        )


def in_twos(rows, work):
    first, last = rows

    def two(number, carry):
        row = first + 2 * number
        work(row)
        work(jnp.minimum(row + 1, last - 1))
        return carry

    lax.fori_loop(0, lax.div(last - first + 1, 2), two, 0)


def lane_sums(values):
    return jnp.sum(jnp.transpose(values), axis=0, keepdims=True)


def separation(place, far):
    apart = [a - b for a, b in zip(place, far)]
    return apart, apart[0] * apart[0] + apart[1] * apart[1] + apart[2] * apart[2]


def kernel_value(radius_sq):
    radius_sq = jnp.maximum(radius_sq, TINY)
    outer = jnp.maximum(1.0 - radius_sq * lax.rsqrt(radius_sq), 0.0)
    twice = outer + outer
    inner = jnp.maximum(twice - 1.0, 0.0)
    return twice * outer * outer - inner * inner * inner


def pair_force(mine, far):
    apart, radius_sq = separation(mine[:3], far[:3])
    speed = [a - b for a, b in zip(mine[3:6], far[3:6])]
    closing = apart[0] * speed[0] + apart[1] * speed[1] + apart[2] * speed[2]
    closing = jnp.minimum(closing, 0.0)
    approach = closing / (radius_sq + SOFTEN)
    viscous = approach * (approach - (mine[7] + far[7])) / (mine[6] + far[6])
    radius_sq = jnp.maximum(radius_sq, TINY)
    inverse = lax.rsqrt(radius_sq)
    radius = radius_sq * inverse
    outer = jnp.maximum(1.0 - radius, 0.0)
    slope = jnp.where(radius < 0.5, 2.0 - 3.0 * radius, outer * outer * inverse)
    return slope * (mine[8] + far[8] + viscous), apart


def density_of(count, steps, list_ref, spread_ref, sum_ref):
    def one_group(group, carry):
        start = pl.multiple_of(group * ROWS, ROWS)
        place = [spread_ref[n, pl.ds(start, ROWS), :] for n in range(3)]

        def one_step(step, total):
            for at in range(CHUNKS):
                chunk = step * CHUNKS + at
                far = [list_ref[chunk, pl.ds(n, 1), :] for n in range(3)]
                weight = list_ref[chunk, pl.ds(6, 1), :]
                total = total + weight * kernel_value(separation(place, far)[1])
            return total

        total = lax.fori_loop(0, steps, one_step, jnp.zeros((ROWS, LANES), jnp.float32))
        sum_ref[pl.ds(start, ROWS), :] = total
        return carry

    lax.fori_loop(0, lax.div(count + ROWS - 1, ROWS), one_group, 0)
    slot = lax.broadcasted_iota(jnp.int32, (1, sum_ref.shape[0]), 1)
    return jnp.where(slot < count, SIGMA * lane_sums(sum_ref[...]), 0.0)


def force_of(count, steps, list_ref, state_list_ref, spread_ref, sum_ref):
    def one_group(group, carry):
        start = pl.multiple_of(group * ROWS, ROWS)

        def one_step(step, total):
            mine = [spread_ref[n, pl.ds(start, ROWS), :] for n in range(9)]
            for at in range(CHUNKS):
                chunk = step * CHUNKS + at
                far = [list_ref[chunk, pl.ds(n, 1), :] for n in range(6)]
                far += [state_list_ref[chunk, pl.ds(n, 1), :] for n in range(3)]
                factor, apart = pair_force(mine, far)
                factor = list_ref[chunk, pl.ds(6, 1), :] * factor
                total = tuple(t + factor * a for t, a in zip(total, apart))
            return total

        zero = jnp.zeros((ROWS, LANES), jnp.float32)
        total = lax.fori_loop(0, steps, one_step, (zero, zero, zero))
        for n in range(3):
            sum_ref[n, pl.ds(start, ROWS), :] = total[n]
        return carry

    lax.fori_loop(0, lax.div(count + ROWS - 1, ROWS), one_group, 0)
    slot = lax.broadcasted_iota(jnp.int32, (1, sum_ref.shape[1]), 1)
    return [
        jnp.where(slot < count, 6.0 * SIGMA * lane_sums(sum_ref[n]), 0.0) for n in range(3)
    ]


def folded(values):
    return jnp.sum(values.reshape(-1, 8, values.shape[-1]), axis=0)


def rows_of(chunks, share):
    first, last = share
    return tuple(lax.div(chunks * end + PARTS - 1, PARTS) for end in (first, last))


def pairs_within(chunks, rows, outputs, pair, sum_ref, fold_ref):
    span = fold_ref.shape[1]
    for n in range(outputs):
        fold_ref[n] = jnp.zeros(fold_ref.shape[1:], jnp.float32)

    def one_row(row, carry):
        def one_chunk(chunk, total):
            by_row, by_column = pair(row, chunk, True)
            for n in range(outputs):
                fold_ref[n, chunk] = fold_ref[n, chunk] + folded(by_column[n])
            return tuple(t + v for t, v in zip(total, by_row))

        total = lax.fori_loop(row + 1, chunks, one_chunk, tuple(pair(row, row, False)[0]))
        for n in range(outputs):
            sum_ref[n, row] = total[n]
        return carry

    lax.fori_loop(*rows, one_row, 0)

    def one_turn(number, carry):
        for at in range(2):
            row = rows[0] + number * 2 + at
            valid = row < rows[1]
            row = jnp.minimum(row, span - 1)
            for n in range(outputs):
                sums = folded(jnp.transpose(sum_ref[n, row]))
                fold_ref[n, row] = fold_ref[n, row] + jnp.where(valid, sums, 0.0)
        return carry

    lax.fori_loop(0, (rows[1] - rows[0] + 1) // 2, one_turn, 0)


def unpacked(fold_ref, number, filled, count, slots):
    lane = lax.broadcasted_iota(jnp.int32, (8, LANES), 1)
    base = lax.shift_right_logical(filled, LANE_BITS)
    back = LANES - (filled & (LANES - 1))
    turned = [
        pltpu.roll(fold_ref[number, base + at], back & (LANES - 1), 1) for at in range(slots // LANES + 1)
    ]
    parts = [jnp.where(lane < back, a, b) for a, b in zip(turned[:-1], turned[1:])]
    row = jnp.sum(jnp.concatenate(parts, axis=1), axis=0, keepdims=True)
    slot = lax.broadcasted_iota(jnp.int32, (1, slots), 1)
    return jnp.where(slot < count, row, 0.0)


def cell_place(target, sizes):
    target = jnp.asarray(target, jnp.int32)
    _, size_y, size_z = sizes
    along = lax.div(target, size_z)
    return lax.div(along, size_y), lax.rem(along, size_y), lax.rem(target, size_z)


def own_place(target, sizes):
    along_x, along_y, along_z = cell_place(target, sizes)
    return along_x, along_y, pl.ds(along_z, 1), slice(None)


def state_tile(density, entropy):
    density = jnp.broadcast_to(density, (8, density.shape[-1]))
    entropy = jnp.broadcast_to(entropy, (8, entropy.shape[-1]))
    active = entropy > 0.0
    safe = jnp.where(active, density, 1.0)
    third = jnp.exp(jnp.log(safe) * (1.0 / 3.0))
    sound = jnp.sqrt(GAMMA * entropy) * third
    row = lax.broadcasted_iota(jnp.int32, safe.shape, 0)
    tile = jnp.where(row == 0, 0.25 * safe, jnp.where(row == 1, 0.25 * sound, entropy / third))
    return tile


def pack_kernel(
    count_hbm, position_hbm, velocity_hbm, mass_hbm, entropy_hbm, out_ref, count_out,
    count_ref, position_ref, velocity_ref, mass_ref, entropy_ref, sems,
):
    sources = (count_hbm, position_hbm, velocity_hbm, mass_hbm, entropy_hbm)
    targets = (count_ref, position_ref, velocity_ref, mass_ref, entropy_ref)
    copies = [
        pltpu.make_async_copy(source, target, sems.at[n])
        for n, (source, target) in enumerate(zip(sources, targets))
    ]
    for copy in copies:
        copy.start()
    for copy in copies:
        copy.wait()
    slots = mass_ref.shape[-1]
    slot = lax.broadcasted_iota(jnp.int32, (8, slots), 1)
    for cell, place in enumerate(np.ndindex(mass_ref.shape[:3])):
        count_out[cell] = count_ref[place]
        at = place[:2] + (pl.ds(place[2], 1), slice(None))
        rows = [position_ref[n, *at] + float(place[n]) for n in range(3)]
        rows += [velocity_ref[n, *at] for n in range(3)]
        rows += [mass_ref[at], entropy_ref[at]]
        tile = jnp.concatenate(rows, axis=0)
        out_ref[place] = jnp.where(slot < count_ref[place], tile, 0.0)


def density_own(count_ref, own_ref, out_ref, list_ref, spread_ref, sum_ref, fold_ref, *, share):
    cells, _, slots = own_ref.shape
    counts = [count_ref[c] for c in range(cells)]
    chunks = fill_list(list(enumerate(counts)), [own_ref], [list_ref], [0.0], 1)

    rows = rows_of(chunks, share)

    def one_spread(chunk):
        spread_chunk(list_ref[chunk], (0, 1, 2, 6), spread_ref, chunk)

    in_twos(rows, one_spread)

    def pair(row, chunk, both):
        mine = [spread_ref[n, rows_at(row), :] for n in range(4)]
        far = [list_ref[chunk, pl.ds(n, 1), :] for n in range(3)]
        value = kernel_value(separation(mine[:3], far)[1])
        weight = list_ref[chunk, pl.ds(6, 1), :]
        return [weight * value], [mine[3] * value] if both else None

    pairs_within(chunks, rows, 1, pair, sum_ref, fold_ref)
    filled = jnp.int32(0)
    for cell, count in enumerate(counts):
        out_ref[pl.ds(cell, 1), :] = SIGMA * unpacked(fold_ref, 0, filled, count, slots)
        filled = filled + count


def density_halo(
    count_ref, table_ref, own_ref, *refs, sizes, parts
):
    partial_refs, piece_refs = refs[:parts], refs[parts : parts + 3]
    rho_ref, again_ref, grid_ref, grid_count_ref, lists_ref, spread_ref, sum_ref = refs[
        parts + 3 :
    ]
    slots = own_ref.shape[-1]
    row = lax.broadcasted_iota(jnp.int32, (8, slots), 0)
    for operand, cell, index, away in halo_cells(sizes):
        tile = piece_refs[operand][cell[0], cell[1], cell[2]]
        grid_count_ref[index] = jnp.sum((tile[7:8] > 0.0).astype(jnp.int32))
        for dim in range(3):
            if away[dim]:
                tile = tile + jnp.where(row == dim, float(away[dim] * sizes[dim]), 0.0)
        grid_ref[index] = tile

    def one_target(target):
        cells = [table_ref[target, n] for n in range(table_ref.shape[1])]
        list_ref = lists_ref.at[target]
        steps = fill_list(
            [(c, grid_count_ref[c]) for c in cells], [grid_ref], [list_ref], [0.0]
        )
        spread(own_ref[target], range(3), spread_ref)
        return density_of(count_ref[target], steps, list_ref, spread_ref, sum_ref)

    def one(target, carry):
        total = one_target(target)
        for partial_ref in partial_refs:
            total = total + partial_ref[pl.ds(target, 1), :]
        rho_ref[*own_place(target, sizes)] = total
        again_ref[*own_place(target, sizes)] = total
        return carry

    lax.fori_loop(0, own_ref.shape[0], one, 0)


def force_own(
    count_ref, own_ref, rho_ref, out_ref,
    list_ref, state_ref, state_list_ref, spread_ref, sum_ref, fold_ref, *, share,
):
    cells, _, slots = own_ref.shape
    counts = [count_ref[c] for c in range(cells)]
    for cell in range(cells):
        density = rho_ref[*own_place(cell, rho_ref.shape[:3])]
        state_ref[cell] = state_tile(density, own_ref[cell, pl.ds(7, 1), :])
    chunks = fill_list(
        list(enumerate(counts)), [own_ref, state_ref], [list_ref, state_list_ref], [0.0, 1.0], 1
    )

    rows = rows_of(chunks, share)

    def one_spread(chunk):
        spread_chunk(list_ref[chunk], range(7), spread_ref, chunk)
        spread_chunk(state_list_ref[chunk], range(3), spread_ref, chunk, 7)

    in_twos(rows, one_spread)

    def pair(row, chunk, both):
        mine = [spread_ref[n, rows_at(row), :] for n in (0, 1, 2, 3, 4, 5, 7, 8, 9)]
        far = [list_ref[chunk, pl.ds(n, 1), :] for n in range(6)]
        far += [state_list_ref[chunk, pl.ds(n, 1), :] for n in range(3)]
        factor, apart = pair_force(mine, far)
        weight = list_ref[chunk, pl.ds(6, 1), :] * factor
        by_row = [weight * a for a in apart]
        if not both:
            return by_row, None
        weight = spread_ref[6, rows_at(row), :] * factor
        return by_row, [-(weight * a) for a in apart]

    pairs_within(chunks, rows, 3, pair, sum_ref, fold_ref)
    for n in range(3):
        filled = jnp.int32(0)
        for cell, count in enumerate(counts):
            out_ref[n, pl.ds(cell, 1), :] = (6.0 * SIGMA) * unpacked(
                fold_ref, n, filled, count, slots
            )
            filled = filled + count


def force_halo(
    count_ref, table_ref, own_ref, density_ref, grid_count_ref, grid_ref, lists_ref,
    *refs, sizes, parts,
):
    partial_refs, piece_refs = refs[:parts], refs[parts : parts + 3]
    out_ref, state_ref, state_list_ref, spread_ref, sum_ref = refs[parts + 3 :]
    for operand, cell, index, _ in halo_cells(sizes):
        density = piece_refs[operand][cell[0], cell[1], pl.ds(cell[2], 1), :]
        state_ref[index] = state_tile(density, grid_ref[index, pl.ds(7, 1), :])

    def one_target(target):
        cells = [table_ref[target, n] for n in range(table_ref.shape[1])]
        steps = fill_list(
            [(c, grid_count_ref[c]) for c in cells], [state_ref], [state_list_ref], [1.0]
        )
        spread(own_ref[target], range(6), spread_ref)
        density = density_ref[*own_place(target, sizes)]
        spread(state_tile(density, own_ref[target, pl.ds(7, 1), :]), range(3), spread_ref, 6)
        return force_of(
            count_ref[target], steps, lists_ref.at[target], state_list_ref, spread_ref, sum_ref
        )

    def one(target, carry):
        sums = one_target(target)
        for n in range(3):
            total = sums[n]
            for partial_ref in partial_refs:
                total = total + partial_ref[n, pl.ds(target, 1), :]
            out_ref[n, *own_place(target, sizes)] = total
        return carry

    lax.fori_loop(0, own_ref.shape[0], one, 0)


def cost(pairs, flops):
    return pl.CostEstimate(flops=pairs * flops, transcendentals=pairs, bytes_accessed=1 << 20)


def per_device(positions, velocities, masses, entropy, counts):
    sizes = masses.shape[:3]
    slots = masses.shape[3]
    cells = sizes[0] * sizes[1] * sizes[2]
    wide = (sizes[0] + 2) * (sizes[1] + 2) * (sizes[2] + 2)
    assert all(size <= 2 for size in sizes)
    packed, own_counts = pl.pallas_call(
        pack_kernel,
        out_shape=(
            jax.ShapeDtypeStruct(sizes + (8, slots), jnp.float32),
            jax.ShapeDtypeStruct((cells,), jnp.int32),
        ),
        in_specs=[pl.BlockSpec(memory_space=pltpu.HBM)] * 5,
        out_specs=(VMEM, SMEM),
        scratch_shapes=[
            pltpu.SMEM(counts.shape, jnp.int32),
            pltpu.VMEM(positions.shape, jnp.float32),
            pltpu.VMEM(velocities.shape, jnp.float32),
            pltpu.VMEM(masses.shape, jnp.float32),
            pltpu.VMEM(entropy.shape, jnp.float32),
            pltpu.SemaphoreType.DMA((5,)),
        ],
        compiler_params=PARAMS,
        name="pack",
    )(
        *(
            pltpu.with_memory_space_constraint(item, pltpu.HBM)
            for item in (counts, positions, velocities, masses, entropy)
        )
    )
    own = packed.reshape(cells, 8, slots)
    table = jnp.asarray(halo_table(sizes))
    near = table.shape[1]
    pairs = cells * slots * slots
    own_chunks = cells * slots // LANES + 2

    def own_rows(fields):
        return pltpu.VMEM((fields, own_chunks, LANES, LANES), jnp.float32)

    def own_spread(fields):
        return pltpu.VMEM((fields, own_chunks * LANES + PAD, LANES), jnp.float32)

    def own_folds(outputs):
        return pltpu.VMEM((outputs, own_chunks, 8, LANES), jnp.float32)

    spread3 = pltpu.VMEM((3, slots + PAD, LANES), jnp.float32)
    spread9 = pltpu.VMEM((9, slots + PAD, LANES), jnp.float32)
    sums = pltpu.VMEM((slots, LANES), jnp.float32)
    three_sums = pltpu.VMEM((3, slots, LANES), jnp.float32)
    own_list = list_scratch(cells, slots)
    halo_list = list_scratch(near, slots)

    partials = [pl.pallas_call(
        functools.partial(density_own, share=share),
        out_shape=jax.ShapeDtypeStruct((cells, slots), jnp.float32),
        in_specs=[SMEM, VMEM],
        out_specs=VMEM,
        scratch_shapes=[own_list, own_spread(4), own_rows(1), own_folds(1)],
        compiler_params=DENSITY_PARAMS,
        cost_estimate=cost(pairs * cells, 22),
    )(own_counts, own) for share in DENSITY_SHARES]
    pieces = with_halo(packed, ORDER)
    result, density, grid, grid_counts, lists = pl.pallas_call(
        functools.partial(density_halo, sizes=sizes, parts=len(DENSITY_SHARES)),
        out_shape=(
            jax.ShapeDtypeStruct(masses.shape, jnp.float32),
            jax.ShapeDtypeStruct(masses.shape, jnp.float32),
            jax.ShapeDtypeStruct((wide, 8, slots), jnp.float32),
            jax.ShapeDtypeStruct((wide,), jnp.int32),
            jax.ShapeDtypeStruct((cells,) + halo_list.shape, jnp.float32),
        ),
        in_specs=[SMEM, SMEM] + [VMEM] * (4 + len(DENSITY_SHARES)),
        out_specs=(VMEM, VMEM, VMEM, SMEM, VMEM),
        scratch_shapes=[spread3, sums],
        compiler_params=DENSITY_PARAMS,
        cost_estimate=cost(pairs * near, 22),
        name="density_halo",
    )(own_counts, table, own, *partials, *pieces)
    partials = [pl.pallas_call(
        functools.partial(force_own, share=share),
        out_shape=jax.ShapeDtypeStruct((3, cells, slots), jnp.float32),
        in_specs=[SMEM, VMEM, VMEM],
        out_specs=VMEM,
        scratch_shapes=[
            own_list, pltpu.VMEM((cells, 8, slots), jnp.float32), own_list,
            own_spread(10), own_rows(3), own_folds(3),
        ],
        compiler_params=PARAMS,
        cost_estimate=cost(pairs * cells, 50),
    )(own_counts, own, density) for share in FORCE_SHARES]
    pieces = with_halo(density, ORDER)
    acceleration = pl.pallas_call(
        functools.partial(force_halo, sizes=sizes, parts=len(FORCE_SHARES)),
        out_shape=jax.ShapeDtypeStruct(positions.shape, jnp.float32),
        in_specs=[SMEM, SMEM, VMEM, VMEM, SMEM] + [VMEM] * (5 + len(FORCE_SHARES)),
        out_specs=VMEM,
        scratch_shapes=[
            pltpu.VMEM((wide, 8, slots), jnp.float32), halo_list,
            spread9, three_sums,
        ],
        compiler_params=PARAMS,
        cost_estimate=cost(pairs * near, 50),
        name="force_halo",
    )(own_counts, table, own, density, grid_counts, grid, lists, *partials, *pieces)
    return (result, acceleration)


def solution(mesh):
    return jax.shard_map(
        per_device,
        mesh=mesh,
        in_specs=(
            P(None, "gx", "gy", "gz", None),
            P(None, "gx", "gy", "gz", None),
            P("gx", "gy", "gz", None),
            P("gx", "gy", "gz", None),
            P("gx", "gy", "gz"),
        ),
        out_specs=(P("gx", "gy", "gz", None), P(None, "gx", "gy", "gz", None)),
        check_vma=False,
    )
```
